32 devices in a mesh: dp: 16 (over z, x, core), mp: 2 (over y).
Axes of the slice: x: 2, y: 2, z: 4, core: 2. Of those that a mesh axis runs over, the one named last changes fastest.
Arguments:
- context: bfloat16 [5120, 2048], P('dp', 'mp'), may hold values from -6 to 6
- out_weight: bfloat16 [2048, 3584], P('mp'), may hold values from -0.125 to 0.125
- cotangent: bfloat16 [5120, 3584], P('dp'), may hold values from -0.059814453 to 0.059814453
- norm_gain: float32 [3584], replicated, may hold values from 0.5 to 1.5
- first_moment: float32 [2, 1024, 3584], P('mp', 'dp'), may hold values from -6 to 6
- second_moment: float32 [2, 1024, 3584], P('mp', 'dp'), may hold values from 0.01 to 1
Outputs:
- new_weight: bfloat16 [2, 1024, 3584], P('mp', 'dp')
- new_first: float32 [2, 1024, 3584], P('mp', 'dp')
- new_second: float32 [2, 1024, 3584], P('mp', 'dp')
- grad_gain: float32 [3584], replicated
- grad_context: bfloat16 [5120, 2048], P('dp', 'mp')
The draws below stay inside these ranges and needn't reach their ends.
All inputs are finite; a program needn't handle non-finite values.
Results may differ from the reference program's by a relative error of at most 0.005.
Values may be sent and summed in bfloat16 or wider, within the bound.
A program may use at most 128 MiB of HBM per device.

```python
import math
import jax
import jax.numpy as jnp
from jax import lax

D = 3584
HQ = 2048
TOKENS = 5120
N_MP = 2


def with_spikes(result, own_key, source, target, parts, factor):
    def block_of(position):
        return (jnp.arange(result.shape[position]) // (result.shape[position] // parts)).reshape((-1,) + (1,) * (result.ndim - 1 - position))

    one_side = jax.random.permutation(own_key, parts)[block_of(target)]
    second = (block_of(target) + parts // 2) % parts
    return jnp.where((block_of(source) == one_side) | (block_of(source) == second), factor * result, result)


def shard_levels(stream_key, extent, split, least, high):
    gain, own = 1.0, jax.random.fold_in(stream_key, 6)
    for position, blocks in split:
        steps = jnp.exp(jax.random.uniform(jax.random.fold_in(own, position), (blocks,), jnp.float32, least / len(split), high / len(split)))
        gain = gain * jnp.repeat(steps, extent[position] // blocks).reshape([-1 if axis == position else 1 for axis in range(len(extent))])
    return gain


def centred(key, extent, spread, reach, pieces=(), dtype=jnp.bfloat16):
    gain = shard_levels(key, extent, pieces, -0.22, 0.18) if pieces else 1.0
    entries = jax.random.normal(key, extent, jnp.float32) * spread * gain
    return jnp.minimum(jnp.maximum(entries, -reach), reach).astype(dtype)


def gaussian_with(own_key, shape, width, limit, cuts, heavy, held_as=jnp.bfloat16):
    array = width * jax.random.normal(own_key, shape, jnp.float32)
    if cuts:
        array = array * shard_levels(own_key, shape, cuts, -0.22, 0.18)
    return jnp.clip(with_spikes(array, jax.random.fold_in(own_key, 3), *heavy), -limit, limit).astype(held_as)


def setup_inputs(seed: int = 0) -> dict:
    arg_keys = jax.random.split(jax.random.key(seed), 7)
    return {
        "context": gaussian_with(arg_keys[0], (TOKENS, HQ), 1.0, 6.0, ((0, 16), (1, 2)), (0, 1, 16, 2.0)),
        "out_weight": centred(arg_keys[1], (HQ, D), HQ ** -0.5, 0.125, ((0, 2),)),
        "cotangent": centred(arg_keys[2], (TOKENS, D), 0.01, 0.059814453, ((0, 16),)),
        "norm_gain": jnp.clip(1.0 + 0.1 * jax.random.normal(arg_keys[3], (D,), jnp.float32), 0.5, 1.5),
        "first_moment": centred(arg_keys[4], (N_MP, HQ // N_MP, D), 1.0, 6.0, ((0, 2), (1, 16)), jnp.float32),
        "second_moment": jnp.clip(jnp.exp(math.log(1.0) - 4.6051702 * jax.random.uniform(arg_keys[5], (N_MP, HQ // N_MP, D), jnp.float32) ** shard_levels(arg_keys[5], (N_MP, HQ // N_MP, D), ((0, 2), (1, 16)), -0.2, 0.2)), 0.01, 1.0),
    }


norm_floor = 0.1
learn_rate = 0.01
beta_one = 0.9
beta_two = 0.95
adam_floor = 1e-08

def reference(context, out_weight, cotangent, norm_gain, first_moment, second_moment):
    attn = jnp.dot(context, out_weight, preferred_element_type=jnp.float32)
    inverse = lax.rsqrt(lax.optimization_barrier(jnp.mean(attn * attn, axis=-1, keepdims=True)) + norm_floor)
    normed = attn * inverse
    upstream = cotangent.astype(jnp.float32)
    scaled = upstream * norm_gain
    grad_gain = lax.optimization_barrier(jnp.sum(upstream * normed, axis=0))
    grad_attn = (inverse * (scaled - normed * lax.optimization_barrier(jnp.mean(scaled * normed, axis=-1, keepdims=True)))).astype(jnp.bfloat16)
    grad_context = jnp.dot(grad_attn, out_weight.T, preferred_element_type=jnp.float32).astype(jnp.bfloat16)
    grad_weight = jnp.dot(context.T, grad_attn, preferred_element_type=jnp.float32)
    grad_weight = grad_weight.reshape(N_MP, HQ // N_MP, D)
    new_first = beta_one * first_moment + (1.0 - beta_one) * grad_weight
    new_second = beta_two * second_moment + (1.0 - beta_two) * grad_weight * grad_weight
    master = out_weight.astype(jnp.float32).reshape(N_MP, HQ // N_MP, D)
    new_weight = (master - learn_rate * new_first / (jnp.sqrt(new_second) + adam_floor)).astype(jnp.bfloat16)
    return (new_weight, new_first, new_second, grad_gain, grad_context)
```

```python
import functools

import jax
import jax.numpy as jnp
from jax import lax
from jax.experimental import pallas as pl
from jax.experimental.pallas import tpu as pltpu
from jax.sharding import PartitionSpec as P

norm_floor = 0.1
learn_rate = 0.01
beta_one = 0.9
beta_two = 0.95
adam_floor = 1e-08

MESH = pl.DeviceIdType.MESH
F32 = jnp.float32
BF16 = jnp.bfloat16
LAG = 2


def kernel(
    cfg,
    ctx_hbm, w_hbm, cot_hbm, gain_hbm, m1_hbm, m2_hbm,
    nw_hbm, n1_hbm, n2_hbm, gg_hbm, gc_hbm,
    wv, ctx, ctxt_all, ctxt, cot, gain, psend, precv, own, stat_s, stat_r, g,
    sends, recvs, keeps, m1, m2, master, nw, gc_acc, gc_out,
    gp, gpr, gfin,
    in_sem, w_sem, cot_sem, m_sem, out_sem, gc_sem, gg_sem,
    ps_s, ps_r, st_s, st_r, cx_s, cx_r, gy_s, gy_r, gm_s, gm_r,
    rs_s, rs_r, gg_s, gg_r,
):
    n, bits, half, chunks, cw, rows, tok, heads, width = cfg
    dp, mp = lax.axis_index("dp"), lax.axis_index("mp")
    peer = 1 - mp

    def flip(index, bit):
        return index + (1 << bit) * (1 - 2 * ((index // (1 << bit)) % 2))

    def peer_id():
        return (dp, peer)

    def bit_id(bit):
        return (flip(dp, bit), mp)

    def column(r):
        first = jnp.where(r < half, mp * half + r, peer * half + r - half)
        return pl.multiple_of(first * cw, cw)

    def ctx_copy():
        return pltpu.make_async_copy(ctx_hbm, ctx.at[pl.ds(0, tok)], in_sem.at[0])

    def gain_copy():
        return pltpu.make_async_copy(gain_hbm.at[pl.ds(mp * half, half)], gain, in_sem.at[1])

    def w_copy(r):
        return pltpu.make_async_copy(w_hbm.at[:, pl.ds(column(r), cw)], wv.at[r], w_sem.at[r])

    def cot_copy(r):
        return pltpu.make_async_copy(cot_hbm.at[:, pl.ds(column(r), cw)], cot.at[r], cot_sem.at[r])

    def m_copies(r):
        cols = pl.ds(column(r), cw)
        return (
            pltpu.make_async_copy(m1_hbm.at[0, :, cols], m1.at[r], m_sem.at[0, r]),
            pltpu.make_async_copy(m2_hbm.at[0, :, cols], m2.at[r], m_sem.at[1, r]),
            pltpu.make_async_copy(
                w_hbm.at[pl.ds(pl.multiple_of(dp * rows, rows), rows), cols], master.at[r], m_sem.at[2, r]
            ),
        )

    def out_copies(r):
        cols = pl.ds(column(r), cw)
        return (
            pltpu.make_async_copy(nw.at[r], nw_hbm.at[0, :, cols], out_sem.at[0, r]),
            pltpu.make_async_copy(m1.at[r], n1_hbm.at[0, :, cols], out_sem.at[1, r]),
            pltpu.make_async_copy(m2.at[r], n2_hbm.at[0, :, cols], out_sem.at[2, r]),
        )

    def remote(src, dst, send_sem, recv_sem, device):
        return pltpu.make_async_remote_copy(
            src_ref=src, dst_ref=dst, send_sem=send_sem, recv_sem=recv_sem,
            device_id=device, device_id_type=MESH,
        )

    def partial_send(c):
        return remote(psend.at[c], precv.at[c], ps_s.at[c], ps_r.at[c], peer_id())

    def stat_send():
        return remote(stat_s, stat_r, st_s, st_r, peer_id())

    def ctx_send():
        return remote(ctx.at[pl.ds(0, tok)], ctx.at[pl.ds(tok, tok)], cx_s, cx_r, bit_id(0))

    def grad_peer(c):
        return remote(
            g.at[c, pl.ds(0, tok)], g.at[half + c, pl.ds(0, tok)], gy_s.at[c], gy_r.at[c], peer_id()
        )

    def grad_mate(r):
        return remote(
            g.at[r, pl.ds(0, tok)], g.at[r, pl.ds(tok, tok)], gm_s.at[r], gm_r.at[r], bit_id(0)
        )

    def shard_send(k, c):
        return remote(
            sends[k - 1].at[c], recvs[k - 1].at[c], rs_s.at[k - 1, c], rs_r.at[k - 1, c], bit_id(k)
        )

    def gain_send(b):
        device = bit_id(b) if b < bits else peer_id()
        return remote(gp.at[b], gpr.at[b], gg_s.at[b], gg_r.at[b], device)

    ctx_copy().start()

    @pl.loop(0, half)
    def _(c):
        w_copy(half + c).start()

    @pl.loop(0, half)
    def _(c):
        w_copy(c).start()
        cot_copy(c).start()

    gain_copy().start()

    @pl.loop(0, chunks)
    def _(r):
        for copy in m_copies(r):
            copy.start()

    barrier = pltpu.get_barrier_semaphore()
    pl.semaphore_signal(barrier, inc=1, device_id=peer_id(), device_id_type=MESH)
    for bit in range(bits):
        pl.semaphore_signal(barrier, inc=1, device_id=bit_id(bit), device_id_type=MESH)
    pl.semaphore_wait(barrier, bits + 1)

    ctx_copy().wait()
    ctx_send().start()

    @pl.loop(0, half)
    def _(c):
        w_copy(half + c).wait()
        psend[c] = jnp.dot(
            ctx[0:tok], wv[half + c], preferred_element_type=F32
        ).astype(BF16)
        partial_send(c).start()

    @pl.loop(0, half)
    def _(c):
        w_copy(c).wait()
        own[c] = jnp.dot(ctx[0:tok], wv[c], preferred_element_type=F32)
        cot_copy(c).wait()

    gain_copy().wait()

    ctx_send().wait_recv()
    ctxt_all[...] = jnp.transpose(ctx[...].astype(F32)).reshape(n, rows, 2 * tok)
    blocks = []
    for place in range(n // 2):
        shard = dp
        for k in range(1, bits):
            if not (place >> (bits - 1 - k)) & 1:
                shard = flip(shard, k)
        blocks.append(ctxt_all[shard])
    ctxt[...] = jnp.concatenate(blocks, axis=0).astype(BF16)

    def fold(value):
        total = value[:, 0:128]
        for lane in range(128, cw, 128):
            total = total + value[:, lane:lane + 128]
        return total

    def gather_stats(c, carry):
        square, cross = carry
        partial_send(c).wait_recv()
        attn = own[c] + precv[c].astype(F32)
        own[c] = attn
        scaled = cot[c].astype(F32) * gain[c]
        return square + fold(attn * attn), cross + fold(scaled * attn)

    zero = jnp.zeros((tok, 128), F32)
    square, cross = lax.fori_loop(0, half, gather_stats, (zero, zero))
    square = jnp.sum(square, axis=1, keepdims=True)
    cross = jnp.sum(cross, axis=1, keepdims=True)
    even = lax.broadcasted_iota(jnp.int32, (tok, 128), 1) % 2 == 0
    stat_s[...] = jnp.transpose(jnp.where(even, square, cross))[0:8]
    stat_send().start()
    stat_send().wait_recv()
    totals = jnp.transpose(jnp.concatenate([stat_s[...] + stat_r[...]] * 16, axis=0))
    inverse = lax.rsqrt(totals[:, 0:1] / width + norm_floor)
    shift = inverse * totals[:, 1:2] / width

    @pl.loop(0, half)
    def _(c):
        upstream = cot[c].astype(F32)
        normed = own[c] * inverse
        g[c, 0:tok] = (inverse * (upstream * gain[c] - normed * shift)).astype(BF16)
        grad_peer(c).start()
        grad_mate(c).start()
        gp[0, c] = jnp.sum(upstream * normed, axis=0, keepdims=True)

    gc_acc[...] = jnp.zeros_like(gc_acc)
    gain_send(0).start()

    n_final = chunks + LAG * (bits - 1)

    @pl.loop(0, max(n_final, bits + 3))
    def _(t):
        ahead = t + 1

        @pl.when((ahead >= half) & (ahead < chunks))
        def _():
            grad_peer(ahead - half).wait_recv()
            grad_mate(ahead).start()

        @pl.when(t < chunks)
        def _():
            grad_mate(t).wait_recv()
            product = jnp.dot(ctxt[...], g[t], preferred_element_type=F32)
            cut = product.shape[0] // 2
            sends[0][t] = product[:cut].astype(BF16)
            shard_send(1, t).start()
            keeps[0][t] = product[cut:]
            gc_acc[...] += lax.dot_general(
                g[t, 0:tok], wv[t], (((1,), (1,)), ((), ())), preferred_element_type=F32
            )

        @pl.when(t == chunks)
        def _():
            gc_out[...] = gc_acc[...].astype(BF16)
            pltpu.make_async_copy(gc_out, gc_hbm, gc_sem).start()

        for b in range(bits + 1):
            @pl.when(t == b + 1)
            def _():
                gain_send(b).wait_recv()
                if b < bits:
                    gp[b + 1] = gp[b] + gpr[b]
                    gain_send(b + 1).start()
                else:
                    gfin[pl.ds(mp * half, half)] = gp[bits]
                    gfin[pl.ds(peer * half, half)] = gpr[bits]
                    pltpu.make_async_copy(gfin, gg_hbm, gg_sem).start()

        for k in range(bits - 1, 0, -1):
            c = t - LAG * k

            @pl.when((c >= 0) & (c < chunks))
            def _():
                shard_send(k, c).wait_recv()
                total = keeps[k - 1][c] + recvs[k - 1][c].astype(F32)
                if k < bits - 1:
                    cut = total.shape[0] // 2
                    sends[k][c] = total[:cut].astype(BF16)
                    shard_send(k + 1, c).start()
                    keeps[k][c] = total[cut:]
                else:
                    for copy in m_copies(c):
                        copy.wait()
                    first = beta_one * m1[c] + (1.0 - beta_one) * total
                    second = beta_two * m2[c] + (1.0 - beta_two) * total * total
                    nw[c] = (
                        master[c].astype(F32) - learn_rate * first / (jnp.sqrt(second) + adam_floor)
                    ).astype(BF16)
                    m1[c] = first
                    m2[c] = second
                    for copy in out_copies(c):
                        copy.start()

    ctx_send().wait_send()
    stat_send().wait_send()

    @pl.loop(0, half)
    def _(c):
        partial_send(c).wait_send()
        grad_peer(c).wait_send()

    for b in range(bits + 1):
        gain_send(b).wait_send()

    @pl.loop(0, chunks)
    def _(r):
        grad_mate(r).wait_send()
        for k in range(1, bits):
            shard_send(k, r).wait_send()
        for copy in out_copies(r):
            copy.wait()

    pltpu.make_async_copy(gc_out, gc_hbm, gc_sem).wait()
    pltpu.make_async_copy(gfin, gg_hbm, gg_sem).wait()


def per_device(n, context, out_weight, cotangent, norm_gain, first_moment, second_moment):
    tok, heads = context.shape
    width = out_weight.shape[1]
    rows = first_moment.shape[1]
    bits = n.bit_length() - 1
    cw = 256
    half = width // (2 * cw)
    chunks = 2 * half
    cfg = (n, bits, half, chunks, cw, rows, tok, heads, width)
    sizes = [(n >> (k + 1)) * rows for k in range(1, bits)]
    dma = pltpu.SemaphoreType.DMA
    vmem = pltpu.VMEM
    scratch = [
        vmem((chunks, heads, cw), BF16),
        vmem((2 * tok, heads), BF16),
        vmem((n, rows, 2 * tok), F32),
        vmem((heads // 2, 2 * tok), BF16),
        vmem((half, tok, cw), BF16),
        vmem((half, 1, cw), F32),
        vmem((half, tok, cw), BF16),
        vmem((half, tok, cw), BF16),
        vmem((half, tok, cw), F32),
        vmem((8, tok), F32),
        vmem((8, tok), F32),
        vmem((chunks, 2 * tok, cw), BF16),
        tuple(vmem((chunks, size, cw), BF16) for size in sizes),
        tuple(vmem((chunks, size, cw), BF16) for size in sizes),
        tuple(vmem((chunks, size, cw), F32) for size in sizes),
        vmem((chunks, rows, cw), F32),
        vmem((chunks, rows, cw), F32),
        vmem((chunks, rows, cw), BF16),
        vmem((chunks, rows, cw), BF16),
        vmem((tok, heads), F32),
        vmem((tok, heads), BF16),
        vmem((bits + 1, half, 1, cw), F32),
        vmem((bits + 1, half, 1, cw), F32),
        vmem((chunks, 1, cw), F32),
        dma((2,)), dma((chunks,)), dma((half,)), dma((3, chunks)), dma((3, chunks)), dma, dma,
        dma((half,)), dma((half,)), dma, dma, dma, dma,
        dma((half,)), dma((half,)), dma((chunks,)), dma((chunks,)),
        dma((bits - 1, chunks)), dma((bits - 1, chunks)), dma((bits + 1,)), dma((bits + 1,)),
    ]
    anywhere = pl.BlockSpec(memory_space=pl.ANY)
    new_weight, new_first, new_second, grad_gain, grad_context = pl.pallas_call(
        functools.partial(kernel, cfg),
        out_shape=(
            jax.ShapeDtypeStruct(first_moment.shape, BF16),
            jax.ShapeDtypeStruct(first_moment.shape, F32),
            jax.ShapeDtypeStruct(first_moment.shape, F32),
            jax.ShapeDtypeStruct((chunks, 1, cw), F32),
            jax.ShapeDtypeStruct((tok, heads), BF16),
        ),
        in_specs=[anywhere] * 6,
        out_specs=(anywhere,) * 5,
        scratch_shapes=scratch,
        compiler_params=pltpu.CompilerParams(
            collective_id=0, has_side_effects=True, vmem_limit_bytes=60 * 1024 * 1024
        ),
    )(context, out_weight, cotangent, norm_gain.reshape(chunks, 1, cw), first_moment, second_moment)
    return (new_weight, new_first, new_second, grad_gain.reshape(width), grad_context)


def solution(mesh):
    return jax.shard_map(
        functools.partial(per_device, mesh.shape["dp"]),
        mesh=mesh,
        in_specs=(
            P("dp", "mp"),
            P("mp", None),
            P("dp", None),
            P(),
            P("mp", "dp", None),
            P("mp", "dp", None),
        ),
        out_specs=(
            P("mp", "dp", None),
            P("mp", "dp", None),
            P("mp", "dp", None),
            P(),
            P("dp", "mp"),
        ),
        check_vma=False,
    )
```

```python
import functools

import jax
import jax.numpy as jnp
from jax import lax
from jax.experimental import pallas as pl
from jax.experimental.pallas import tpu as pltpu
from jax.sharding import PartitionSpec as P

norm_floor = 0.1
learn_rate = 0.01
beta_one = 0.9
beta_two = 0.95
adam_floor = 1e-08

MESH = pl.DeviceIdType.MESH
F32 = jnp.float32
BF16 = jnp.bfloat16
LAG = 2


def kernel(
    cfg,
    ctx_hbm, w_hbm, cot_hbm, gain_hbm, m1_hbm, m2_hbm,
    nw, n1, n2, gfin, gc_out,
    wv, ctx, ctxt_all, ctxt, cot, gain_flat, gain, psend, precv, own, stat_s, stat_r, g,
    sends, recvs, keeps, m1, m2, master, gc_acc,
    gp, gpr,
    in_sem, w_sem, cot_sem, m_sem,
    ps_s, ps_r, st_s, st_r, cx_s, cx_r, gy_s, gy_r, gm_s, gm_r,
    rs_s, rs_r, gg_s, gg_r,
):
    n, bits, half, chunks, cw, rows, tok, heads, width = cfg
    dp, mp = lax.axis_index("dp"), lax.axis_index("mp")
    peer = 1 - mp

    def flip(index, bit):
        return index + (1 << bit) * (1 - 2 * ((index // (1 << bit)) % 2))

    def peer_id():
        return (dp, peer)

    def bit_id(bit):
        return (flip(dp, bit), mp)

    def late(c):
        return c % half == half // 2

    def turn_bits(k):
        return k, k + 1 if k < bits - 1 else 1

    def turn_id(k, c):
        usual, other = turn_bits(k)
        return (jnp.where(late(c), flip(dp, other), flip(dp, usual)), mp)

    def column(r):
        first = jnp.where(r < half, mp * half + r, peer * half + r - half)
        return pl.multiple_of(first * cw, cw)

    def ctx_copy():
        return pltpu.make_async_copy(ctx_hbm, ctx.at[pl.ds(0, tok)], in_sem.at[0])

    def gain_copy():
        return pltpu.make_async_copy(gain_hbm, gain_flat, in_sem.at[1])

    def w_copy(r):
        return pltpu.make_async_copy(w_hbm.at[:, pl.ds(column(r), cw)], wv.at[r], w_sem.at[r])

    def cot_copy(r):
        return pltpu.make_async_copy(cot_hbm.at[:, pl.ds(column(r), cw)], cot.at[r], cot_sem.at[r])

    def m_copies(r):
        cols = pl.ds(column(r), cw)
        return (
            pltpu.make_async_copy(m1_hbm.at[0, :, cols], m1.at[r], m_sem.at[0, r]),
            pltpu.make_async_copy(m2_hbm.at[0, :, cols], m2.at[r], m_sem.at[1, r]),
            pltpu.make_async_copy(
                w_hbm.at[pl.ds(pl.multiple_of(dp * rows, rows), rows), cols], master.at[r], m_sem.at[2, r]
            ),
        )

    def remote(src, dst, send_sem, recv_sem, device):
        return pltpu.make_async_remote_copy(
            src_ref=src, dst_ref=dst, send_sem=send_sem, recv_sem=recv_sem,
            device_id=device, device_id_type=MESH,
        )

    def partial_send(c):
        return remote(psend.at[c], precv.at[c], ps_s.at[c], ps_r.at[c], peer_id())

    def stat_send():
        return remote(stat_s, stat_r, st_s, st_r, peer_id())

    def ctx_send():
        return remote(ctx.at[pl.ds(0, tok)], ctx.at[pl.ds(tok, tok)], cx_s, cx_r, bit_id(0))

    def grad_peer(c):
        return remote(
            g.at[c, pl.ds(0, tok)], g.at[half + c, pl.ds(0, tok)], gy_s.at[c], gy_r.at[c], peer_id()
        )

    def grad_mate(r):
        return remote(
            g.at[r, pl.ds(0, tok)], g.at[r, pl.ds(tok, tok)], gm_s.at[r], gm_r.at[r], bit_id(0)
        )

    def shard_send(k, c):
        return remote(
            sends[k - 1].at[c], recvs[k - 1].at[c], rs_s.at[k - 1, c], rs_r.at[k - 1, c], turn_id(k, c)
        )

    def gain_send(b):
        device = bit_id(b) if b < bits else peer_id()
        return remote(gp.at[b], gpr.at[b], gg_s.at[b], gg_r.at[b], device)

    ctx_copy().start()

    @pl.loop(0, half)
    def _(c):
        w_copy(half + c).start()

    @pl.loop(0, half)
    def _(c):
        w_copy(c).start()
        cot_copy(c).start()

    gain_copy().start()

    @pl.loop(0, chunks)
    def _(r):
        for copy in m_copies(r):
            copy.start()

    barrier = pltpu.get_barrier_semaphore()
    pl.semaphore_signal(barrier, inc=1, device_id=peer_id(), device_id_type=MESH)
    for bit in range(bits):
        pl.semaphore_signal(barrier, inc=1, device_id=bit_id(bit), device_id_type=MESH)
    pl.semaphore_wait(barrier, bits + 1)

    ctx_copy().wait()
    ctx_send().start()

    @pl.loop(0, half)
    def _(c):
        w_copy(half + c).wait()
        psend[c] = jnp.dot(
            ctx[0:tok], wv[half + c], preferred_element_type=F32
        ).astype(BF16)
        partial_send(c).start()

    @pl.loop(0, half)
    def _(c):
        w_copy(c).wait()
        own[c] = jnp.dot(ctx[0:tok], wv[c], preferred_element_type=F32)
        cot_copy(c).wait()

    gain_copy().wait()
    for r in range(chunks):
        gain[r] = gain_flat[r * cw:(r + 1) * cw].reshape(1, cw)

    ctx_send().wait_recv()
    ctxt_all[...] = jnp.transpose(ctx[...].astype(F32)).reshape(n, rows, 2 * tok)
    for order in range(2):
        blocks = []
        for place in range(n // 2):
            shard = dp
            for k in range(1, bits):
                if not (place >> (bits - 1 - k)) & 1:
                    shard = flip(shard, turn_bits(k)[order])
            blocks.append(ctxt_all[shard])
        ctxt[order] = jnp.concatenate(blocks, axis=0).astype(BF16)

    def fold(value):
        total = value[:, 0:128]
        for lane in range(128, cw, 128):
            total = total + value[:, lane:lane + 128]
        return total

    def gather_stats(c, carry):
        square, cross = carry
        partial_send(c).wait_recv()
        attn = own[c] + precv[c].astype(F32)
        own[c] = attn
        scaled = cot[c].astype(F32) * gain[mp * half + c]
        return square + fold(attn * attn), cross + fold(scaled * attn)

    zero = jnp.zeros((tok, 128), F32)
    square, cross = lax.fori_loop(0, half, gather_stats, (zero, zero))
    square = jnp.sum(square, axis=1, keepdims=True)
    cross = jnp.sum(cross, axis=1, keepdims=True)
    even = lax.broadcasted_iota(jnp.int32, (tok, 128), 1) % 2 == 0
    stat_s[...] = jnp.transpose(jnp.where(even, square, cross))[0:8]
    stat_send().start()
    stat_send().wait_recv()
    totals = jnp.transpose(jnp.concatenate([stat_s[...] + stat_r[...]] * 16, axis=0))
    inverse = lax.rsqrt(totals[:, 0:1] / width + norm_floor)
    shift = inverse * totals[:, 1:2] / width

    @pl.loop(0, half)
    def _(c):
        upstream = cot[c].astype(F32)
        normed = own[c] * inverse
        g[c, 0:tok] = (inverse * (upstream * gain[mp * half + c] - normed * shift)).astype(BF16)
        grad_peer(c).start()
        grad_mate(c).start()
        gp[0, c] = jnp.sum(upstream * normed, axis=0, keepdims=True)

    gc_acc[...] = jnp.zeros_like(gc_acc)
    gain_send(0).start()

    n_final = chunks + LAG * (bits - 1)

    @pl.loop(0, max(n_final, bits + 3))
    def _(t):
        ahead = t + 1

        @pl.when((ahead >= half) & (ahead < chunks))
        def _():
            grad_peer(ahead - half).wait_recv()
            grad_mate(ahead).start()

        @pl.when(t < chunks)
        def _():
            grad_mate(t).wait_recv()
            product = jnp.dot(ctxt[late(t).astype(jnp.int32)], g[t], preferred_element_type=F32)
            cut = product.shape[0] // 2
            sends[0][t] = product[:cut].astype(BF16)
            shard_send(1, t).start()
            keeps[0][t] = product[cut:]
            gc_acc[...] += lax.dot_general(
                g[t, 0:tok], wv[t], (((1,), (1,)), ((), ())), preferred_element_type=F32
            )

        @pl.when(t == chunks)
        def _():
            gc_out[...] = gc_acc[...].astype(BF16)

        for b in range(bits + 1):
            @pl.when(t == b + 1)
            def _():
                gain_send(b).wait_recv()
                if b < bits:
                    gp[b + 1] = gp[b] + gpr[b]
                    gain_send(b + 1).start()
                else:
                    gfin[pl.ds(mp * half, half)] = gp[bits]
                    gfin[pl.ds(peer * half, half)] = gpr[bits]

        for k in range(bits - 1, 0, -1):
            c = t - LAG * k

            @pl.when((c >= 0) & (c < chunks))
            def _():
                shard_send(k, c).wait_recv()
                total = keeps[k - 1][c] + recvs[k - 1][c].astype(F32)
                if k < bits - 1:
                    cut = total.shape[0] // 2
                    sends[k][c] = total[:cut].astype(BF16)
                    shard_send(k + 1, c).start()
                    keeps[k][c] = total[cut:]
                else:
                    for copy in m_copies(c):
                        copy.wait()
                    first = beta_one * m1[c] + (1.0 - beta_one) * total
                    second = beta_two * m2[c] + (1.0 - beta_two) * total * total
                    cols = pl.ds(column(c), cw)
                    nw[0, :, cols] = (
                        master[c].astype(F32) - learn_rate * first / (jnp.sqrt(second) + adam_floor)
                    ).astype(BF16)
                    n1[0, :, cols] = first
                    n2[0, :, cols] = second

    ctx_send().wait_send()
    stat_send().wait_send()

    @pl.loop(0, half)
    def _(c):
        partial_send(c).wait_send()
        grad_peer(c).wait_send()

    for b in range(bits + 1):
        gain_send(b).wait_send()

    @pl.loop(0, chunks)
    def _(r):
        grad_mate(r).wait_send()
        for k in range(1, bits):
            shard_send(k, r).wait_send()


def settle(nw, n1, n2, gg, gc, nw_out, n1_out, n2_out, gg_out, gc_out, flat, sem):
    pairs = ((nw, nw_out), (n1, n1_out), (n2, n2_out), (gc, gc_out))
    copies = [pltpu.make_async_copy(a, b, sem.at[i]) for i, (a, b) in enumerate(pairs)]
    for copy in copies:
        copy.start()
    chunks, _, cw = gg.shape
    for r in range(chunks):
        flat[r * cw:(r + 1) * cw] = gg[r].reshape(cw)
    copies.append(pltpu.make_async_copy(flat, gg_out, sem.at[4]))
    copies[-1].start()
    for copy in copies:
        copy.wait()


def per_device(n, context, out_weight, cotangent, norm_gain, first_moment, second_moment):
    tok, heads = context.shape
    width = out_weight.shape[1]
    rows = first_moment.shape[1]
    bits = n.bit_length() - 1
    cw = 256
    half = width // (2 * cw)
    chunks = 2 * half
    cfg = (n, bits, half, chunks, cw, rows, tok, heads, width)
    sizes = [(n >> (k + 1)) * rows for k in range(1, bits)]
    dma = pltpu.SemaphoreType.DMA
    vmem = pltpu.VMEM
    scratch = [
        vmem((chunks, heads, cw), BF16),
        vmem((2 * tok, heads), BF16),
        vmem((n, rows, 2 * tok), F32),
        vmem((2, heads // 2, 2 * tok), BF16),
        vmem((half, tok, cw), BF16),
        vmem((width,), F32),
        vmem((chunks, 1, cw), F32),
        vmem((half, tok, cw), BF16),
        vmem((half, tok, cw), BF16),
        vmem((half, tok, cw), F32),
        vmem((8, tok), F32),
        vmem((8, tok), F32),
        vmem((chunks, 2 * tok, cw), BF16),
        tuple(vmem((chunks, size, cw), BF16) for size in sizes),
        tuple(vmem((chunks, size, cw), BF16) for size in sizes),
        tuple(vmem((chunks, size, cw), F32) for size in sizes),
        vmem((chunks, rows, cw), F32),
        vmem((chunks, rows, cw), F32),
        vmem((chunks, rows, cw), BF16),
        vmem((tok, heads), F32),
        vmem((bits + 1, half, 1, cw), F32),
        vmem((bits + 1, half, 1, cw), F32),
        dma((2,)), dma((chunks,)), dma((half,)), dma((3, chunks)),
        dma((half,)), dma((half,)), dma, dma, dma, dma,
        dma((half,)), dma((half,)), dma((chunks,)), dma((chunks,)),
        dma((bits - 1, chunks)), dma((bits - 1, chunks)), dma((bits + 1,)), dma((bits + 1,)),
    ]
    anywhere = pl.BlockSpec(memory_space=pltpu.HBM)
    new_weight, new_first, new_second, grad_gain, grad_context = pl.pallas_call(
        functools.partial(kernel, cfg),
        out_shape=(
            jax.ShapeDtypeStruct(first_moment.shape, BF16),
            jax.ShapeDtypeStruct(first_moment.shape, F32),
            jax.ShapeDtypeStruct(first_moment.shape, F32),
            jax.ShapeDtypeStruct((chunks, 1, cw), F32),
            jax.ShapeDtypeStruct((tok, heads), BF16),
        ),
        in_specs=[anywhere] * 6,
        out_specs=(pl.BlockSpec(memory_space=pltpu.VMEM),) * 5,
        scratch_shapes=scratch,
        compiler_params=pltpu.CompilerParams(
            collective_id=0, has_side_effects=True, vmem_limit_bytes=50 * 1024 * 1024
        ),
    )(context, out_weight, cotangent, norm_gain, first_moment, second_moment)
    return pl.pallas_call(
        settle,
        out_shape=(
            jax.ShapeDtypeStruct(first_moment.shape, BF16),
            jax.ShapeDtypeStruct(first_moment.shape, F32),
            jax.ShapeDtypeStruct(first_moment.shape, F32),
            jax.ShapeDtypeStruct((width,), F32),
            jax.ShapeDtypeStruct((tok, heads), BF16),
        ),
        in_specs=[pl.BlockSpec(memory_space=pltpu.VMEM)] * 5,
        out_specs=(anywhere,) * 5,
        scratch_shapes=[vmem((width,), F32), dma((5,))],
        compiler_params=pltpu.CompilerParams(vmem_limit_bytes=8 * 1024 * 1024),
    )(new_weight, new_first, new_second, grad_gain, grad_context)


def solution(mesh):
    return jax.shard_map(
        functools.partial(per_device, mesh.shape["dp"]),
        mesh=mesh,
        in_specs=(
            P("dp", "mp"),
            P("mp", None),
            P("dp", None),
            P(),
            P("mp", "dp", None),
            P("mp", "dp", None),
        ),
        out_specs=(
            P("mp", "dp", None),
            P("mp", "dp", None),
            P("mp", "dp", None),
            P(),
            P("dp", "mp"),
        ),
        check_vma=False,
    )
```

```python
import functools

import jax
import jax.numpy as jnp
from jax import lax
from jax.experimental import pallas as pl
from jax.experimental.pallas import tpu as pltpu
from jax.sharding import PartitionSpec as P

norm_floor = 0.1
learn_rate = 0.01
beta_one = 0.9
beta_two = 0.95
adam_floor = 1e-08

MESH = pl.DeviceIdType.MESH
F32 = jnp.float32
BF16 = jnp.bfloat16
LAG = 2
AHEAD = 2


def kernel(
    cfg,
    ctx_hbm, w_hbm, cot_hbm, gain_hbm, m1_hbm, m2_hbm,
    nw, n1, n2, gfin, gc_out,
    wv, ctx, ctxt_all, ctxt, cot, gain_flat, gain, psend, precv, own, stat_s, stat_r, g,
    sends, recvs, keeps, m1, m2, master, gc_acc,
    gp, gpr,
    in_sem, w_sem, cot_sem, m_sem,
    ps_s, ps_r, st_s, st_r, cx_s, cx_r, gy_s, gy_r, gm_s, gm_r,
    rs_s, rs_r, gg_s, gg_r,
):
    n, bits, half, chunks, cw, rows, tok, heads, width = cfg
    dp, mp = lax.axis_index("dp"), lax.axis_index("mp")
    peer = 1 - mp

    def flip(index, bit):
        return index + (1 << bit) * (1 - 2 * ((index // (1 << bit)) % 2))

    def peer_id():
        return (dp, peer)

    def bit_id(bit):
        return (flip(dp, bit), mp)

    def column(r):
        first = jnp.where(r < half, mp * half + r, peer * half + r - half)
        return pl.multiple_of(first * cw, cw)

    def ctx_copy():
        return pltpu.make_async_copy(ctx_hbm, ctx.at[pl.ds(0, tok)], in_sem.at[0])

    def gain_copy():
        return pltpu.make_async_copy(gain_hbm, gain_flat, in_sem.at[1])

    def w_copy(r):
        return pltpu.make_async_copy(w_hbm.at[:, pl.ds(column(r), cw)], wv.at[r], w_sem.at[r])

    def cot_copy(r):
        return pltpu.make_async_copy(cot_hbm.at[:, pl.ds(column(r), cw)], cot.at[r], cot_sem.at[r])

    def m_copies(r):
        cols = pl.ds(column(r), cw)
        return (
            pltpu.make_async_copy(m1_hbm.at[0, :, cols], m1.at[r], m_sem.at[0, r]),
            pltpu.make_async_copy(m2_hbm.at[0, :, cols], m2.at[r], m_sem.at[1, r]),
            pltpu.make_async_copy(
                w_hbm.at[pl.ds(pl.multiple_of(dp * rows, rows), rows), cols], master.at[r], m_sem.at[2, r]
            ),
        )

    def remote(src, dst, send_sem, recv_sem, device):
        return pltpu.make_async_remote_copy(
            src_ref=src, dst_ref=dst, send_sem=send_sem, recv_sem=recv_sem,
            device_id=device, device_id_type=MESH,
        )

    def partial_send(c):
        return remote(psend.at[c], precv.at[c], ps_s.at[c], ps_r.at[c], peer_id())

    def stat_send():
        return remote(stat_s, stat_r, st_s, st_r, peer_id())

    def ctx_send():
        return remote(ctx.at[pl.ds(0, tok)], ctx.at[pl.ds(tok, tok)], cx_s, cx_r, bit_id(0))

    def grad_peer(c):
        return remote(
            g.at[c, pl.ds(0, tok)], g.at[half + c, pl.ds(0, tok)], gy_s.at[c], gy_r.at[c], peer_id()
        )

    def grad_mate(r):
        return remote(
            g.at[r, pl.ds(0, tok)], g.at[r, pl.ds(tok, tok)], gm_s.at[r], gm_r.at[r], bit_id(0)
        )

    def shard_send(k, c):
        return remote(
            sends[k - 1].at[c], recvs[k - 1].at[c], rs_s.at[k - 1, c], rs_r.at[k - 1, c], bit_id(k)
        )

    def gain_send(b):
        device = bit_id(b) if b < bits else peer_id()
        return remote(gp.at[b], gpr.at[b], gg_s.at[b], gg_r.at[b], device)

    ctx_copy().start()

    @pl.loop(0, half)
    def _(c):
        w_copy(half + c).start()

    @pl.loop(0, half)
    def _(c):
        w_copy(c).start()
        cot_copy(c).start()

    gain_copy().start()

    @pl.loop(0, chunks)
    def _(r):
        for copy in m_copies(r):
            copy.start()

    barrier = pltpu.get_barrier_semaphore()
    pl.semaphore_signal(barrier, inc=1, device_id=peer_id(), device_id_type=MESH)
    for bit in range(bits):
        pl.semaphore_signal(barrier, inc=1, device_id=bit_id(bit), device_id_type=MESH)
    pl.semaphore_wait(barrier, bits + 1)

    ctx_copy().wait()
    ctx_send().start()

    @pl.loop(0, half)
    def _(c):
        w_copy(half + c).wait()
        psend[c] = jnp.dot(
            ctx[0:tok], wv[half + c], preferred_element_type=F32
        ).astype(BF16)
        partial_send(c).start()

    @pl.loop(0, half)
    def _(c):
        w_copy(c).wait()
        own[c] = jnp.dot(ctx[0:tok], wv[c], preferred_element_type=F32)
        cot_copy(c).wait()

    gain_copy().wait()
    for r in range(chunks):
        gain[r] = gain_flat[r * cw:(r + 1) * cw].reshape(1, cw)

    ctx_send().wait_recv()
    ctxt_all[...] = jnp.transpose(ctx[...].astype(F32)).reshape(n, rows, 2 * tok)
    blocks = []
    for place in range(n // 2):
        shard = dp
        for k in range(1, bits):
            if not (place >> (bits - 1 - k)) & 1:
                shard = flip(shard, k)
        blocks.append(ctxt_all[shard])
    ctxt[...] = jnp.concatenate(blocks, axis=0).astype(BF16)

    def fold(value):
        total = value[:, 0:128]
        for lane in range(128, cw, 128):
            total = total + value[:, lane:lane + 128]
        return total

    def gather_stats(c, carry):
        square, cross = carry
        partial_send(c).wait_recv()
        attn = own[c] + precv[c].astype(F32)
        own[c] = attn
        scaled = cot[c].astype(F32) * gain[mp * half + c]
        return square + fold(attn * attn), cross + fold(scaled * attn)

    zero = jnp.zeros((tok, 128), F32)
    square, cross = lax.fori_loop(0, half, gather_stats, (zero, zero))
    square = jnp.sum(square, axis=1, keepdims=True)
    cross = jnp.sum(cross, axis=1, keepdims=True)
    even = lax.broadcasted_iota(jnp.int32, (tok, 128), 1) % 2 == 0
    stat_s[...] = jnp.transpose(jnp.where(even, square, cross))[0:8]
    stat_send().start()
    stat_send().wait_recv()
    totals = jnp.transpose(jnp.concatenate([stat_s[...] + stat_r[...]] * 16, axis=0))
    inverse = lax.rsqrt(totals[:, 0:1] / width + norm_floor)
    shift = inverse * totals[:, 1:2] / width

    @pl.loop(0, half)
    def _(c):
        upstream = cot[c].astype(F32)
        normed = own[c] * inverse
        g[c, 0:tok] = (inverse * (upstream * gain[mp * half + c] - normed * shift)).astype(BF16)
        grad_peer(c).start()
        grad_mate(c).start()
        gp[0, c] = jnp.sum(upstream * normed, axis=0, keepdims=True)

    gc_acc[...] = jnp.zeros_like(gc_acc)
    gain_send(0).start()

    n_final = chunks + LAG * (bits - 1)

    @pl.loop(0, max(n_final, bits + 3))
    def _(t):
        ahead = t + AHEAD

        @pl.when((ahead >= half) & (ahead < chunks))
        def _():
            grad_peer(ahead - half).wait_recv()
            grad_mate(ahead).start()

        @pl.when(t < chunks)
        def _():
            grad_mate(t).wait_recv()
            product = jnp.dot(ctxt[...], g[t], preferred_element_type=F32)
            cut = product.shape[0] // 2
            sends[0][t] = product[:cut].astype(BF16)
            shard_send(1, t).start()
            keeps[0][t] = product[cut:]
            gc_acc[...] += lax.dot_general(
                g[t, 0:tok], wv[t], (((1,), (1,)), ((), ())), preferred_element_type=F32
            )

        @pl.when(t == chunks)
        def _():
            gc_out[...] = gc_acc[...].astype(BF16)

        for b in range(bits + 1):
            @pl.when(t == b + 1)
            def _():
                gain_send(b).wait_recv()
                if b < bits:
                    gp[b + 1] = gp[b] + gpr[b]
                    gain_send(b + 1).start()
                else:
                    gfin[pl.ds(mp * half, half)] = gp[bits]
                    gfin[pl.ds(peer * half, half)] = gpr[bits]

        for k in range(bits - 1, 0, -1):
            c = t - LAG * k

            @pl.when((c >= 0) & (c < chunks))
            def _():
                shard_send(k, c).wait_recv()
                total = keeps[k - 1][c] + recvs[k - 1][c].astype(F32)
                if k < bits - 1:
                    cut = total.shape[0] // 2
                    sends[k][c] = total[:cut].astype(BF16)
                    shard_send(k + 1, c).start()
                    keeps[k][c] = total[cut:]
                else:
                    for copy in m_copies(c):
                        copy.wait()
                    first = beta_one * m1[c] + (1.0 - beta_one) * total
                    second = beta_two * m2[c] + (1.0 - beta_two) * total * total
                    cols = pl.ds(column(c), cw)
                    nw[0, :, cols] = (
                        master[c].astype(F32) - learn_rate * first / (jnp.sqrt(second) + adam_floor)
                    ).astype(BF16)
                    n1[0, :, cols] = first
                    n2[0, :, cols] = second

    ctx_send().wait_send()
    stat_send().wait_send()

    @pl.loop(0, half)
    def _(c):
        partial_send(c).wait_send()
        grad_peer(c).wait_send()

    for b in range(bits + 1):
        gain_send(b).wait_send()

    @pl.loop(0, chunks)
    def _(r):
        grad_mate(r).wait_send()
        for k in range(1, bits):
            shard_send(k, r).wait_send()


def settle(nw, n1, n2, gg, gc, nw_out, n1_out, n2_out, gg_out, gc_out, flat, sem):
    pairs = ((nw, nw_out), (n1, n1_out), (n2, n2_out), (gc, gc_out))
    copies = [pltpu.make_async_copy(a, b, sem.at[i]) for i, (a, b) in enumerate(pairs)]
    for copy in copies:
        copy.start()
    chunks, _, cw = gg.shape
    for r in range(chunks):
        flat[r * cw:(r + 1) * cw] = gg[r].reshape(cw)
    copies.append(pltpu.make_async_copy(flat, gg_out, sem.at[4]))
    copies[-1].start()
    for copy in copies:
        copy.wait()


def per_device(n, context, out_weight, cotangent, norm_gain, first_moment, second_moment):
    tok, heads = context.shape
    width = out_weight.shape[1]
    rows = first_moment.shape[1]
    bits = n.bit_length() - 1
    cw = 256
    half = width // (2 * cw)
    chunks = 2 * half
    cfg = (n, bits, half, chunks, cw, rows, tok, heads, width)
    sizes = [(n >> (k + 1)) * rows for k in range(1, bits)]
    dma = pltpu.SemaphoreType.DMA
    vmem = pltpu.VMEM
    scratch = [
        vmem((chunks, heads, cw), BF16),
        vmem((2 * tok, heads), BF16),
        vmem((n, rows, 2 * tok), F32),
        vmem((heads // 2, 2 * tok), BF16),
        vmem((half, tok, cw), BF16),
        vmem((width,), F32),
        vmem((chunks, 1, cw), F32),
        vmem((half, tok, cw), BF16),
        vmem((half, tok, cw), BF16),
        vmem((half, tok, cw), F32),
        vmem((8, tok), F32),
        vmem((8, tok), F32),
        vmem((chunks, 2 * tok, cw), BF16),
        tuple(vmem((chunks, size, cw), BF16) for size in sizes),
        tuple(vmem((chunks, size, cw), BF16) for size in sizes),
        tuple(vmem((chunks, size, cw), F32) for size in sizes),
        vmem((chunks, rows, cw), F32),
        vmem((chunks, rows, cw), F32),
        vmem((chunks, rows, cw), BF16),
        vmem((tok, heads), F32),
        vmem((bits + 1, half, 1, cw), F32),
        vmem((bits + 1, half, 1, cw), F32),
        dma((2,)), dma((chunks,)), dma((half,)), dma((3, chunks)),
        dma((half,)), dma((half,)), dma, dma, dma, dma,
        dma((half,)), dma((half,)), dma((chunks,)), dma((chunks,)),
        dma((bits - 1, chunks)), dma((bits - 1, chunks)), dma((bits + 1,)), dma((bits + 1,)),
    ]
    anywhere = pl.BlockSpec(memory_space=pltpu.HBM)
    new_weight, new_first, new_second, grad_gain, grad_context = pl.pallas_call(
        functools.partial(kernel, cfg),
        out_shape=(
            jax.ShapeDtypeStruct(first_moment.shape, BF16),
            jax.ShapeDtypeStruct(first_moment.shape, F32),
            jax.ShapeDtypeStruct(first_moment.shape, F32),
            jax.ShapeDtypeStruct((chunks, 1, cw), F32),
            jax.ShapeDtypeStruct((tok, heads), BF16),
        ),
        in_specs=[anywhere] * 6,
        out_specs=(pl.BlockSpec(memory_space=pltpu.VMEM),) * 5,
        scratch_shapes=scratch,
        compiler_params=pltpu.CompilerParams(
            collective_id=0, has_side_effects=True, vmem_limit_bytes=50 * 1024 * 1024
        ),
    )(context, out_weight, cotangent, norm_gain, first_moment, second_moment)
    return pl.pallas_call(
        settle,
        out_shape=(
            jax.ShapeDtypeStruct(first_moment.shape, BF16),
            jax.ShapeDtypeStruct(first_moment.shape, F32),
            jax.ShapeDtypeStruct(first_moment.shape, F32),
            jax.ShapeDtypeStruct((width,), F32),
            jax.ShapeDtypeStruct((tok, heads), BF16),
        ),
        in_specs=[pl.BlockSpec(memory_space=pltpu.VMEM)] * 5,
        out_specs=(anywhere,) * 5,
        scratch_shapes=[vmem((width,), F32), dma((5,))],
        compiler_params=pltpu.CompilerParams(vmem_limit_bytes=8 * 1024 * 1024),
    )(new_weight, new_first, new_second, grad_gain, grad_context)


def solution(mesh):
    return jax.shard_map(
        functools.partial(per_device, mesh.shape["dp"]),
        mesh=mesh,
        in_specs=(
            P("dp", "mp"),
            P("mp", None),
            P("dp", None),
            P(),
            P("mp", "dp", None),
            P("mp", "dp", None),
        ),
        out_specs=(
            P("mp", "dp", None),
            P("mp", "dp", None),
            P("mp", "dp", None),
            P(),
            P("dp", "mp"),
        ),
        check_vma=False,
    )
```

```python
import functools

import jax
import jax.numpy as jnp
from jax import lax
from jax.experimental import pallas as pl
from jax.experimental.pallas import tpu as pltpu
from jax.sharding import PartitionSpec as P

norm_floor = 0.1
learn_rate = 0.01
beta_one = 0.9
beta_two = 0.95
adam_floor = 1e-08

MESH = pl.DeviceIdType.MESH
F32 = jnp.float32
BF16 = jnp.bfloat16
LAG = 2
AHEAD = 2


def kernel(
    cfg,
    ctx_hbm, w_hbm, cot_hbm, gain_hbm, m1_hbm, m2_hbm,
    nw, n1, n2, gfin, gc_out,
    wv, ctx, ctxt_all, ctxt, cot, gain_flat, gain, psend, precv, own, stat_s, stat_r, g,
    sends, recvs, keeps, m1, m2, master, gc_acc,
    gp, gpr,
    in_sem, w_sem, cot_sem, m_sem,
    ps_s, ps_r, st_s, st_r, cx_s, cx_r, gy_s, gy_r, gm_s, gm_r,
    rs_s, rs_r, gg_s, gg_r,
):
    n, bits, half, chunks, cw, rows, tok, heads, width = cfg
    dp, mp = lax.axis_index("dp"), lax.axis_index("mp")
    peer = 1 - mp

    def flip(index, bit):
        return index + (1 << bit) * (1 - 2 * ((index // (1 << bit)) % 2))

    def peer_id():
        return (dp, peer)

    def bit_id(bit):
        return (flip(dp, bit), mp)

    def column(r):
        first = jnp.where(r < half, mp * half + r, peer * half + r - half)
        return pl.multiple_of(first * cw, cw)

    def ctx_copy():
        return pltpu.make_async_copy(ctx_hbm, ctx.at[pl.ds(0, tok)], in_sem.at[0])

    def gain_copy():
        return pltpu.make_async_copy(gain_hbm, gain_flat, in_sem.at[1])

    def w_copy(r):
        return pltpu.make_async_copy(w_hbm.at[:, pl.ds(column(r), cw)], wv.at[r], w_sem.at[r])

    def cot_copy(r):
        return pltpu.make_async_copy(cot_hbm.at[:, pl.ds(column(r), cw)], cot.at[r], cot_sem.at[r])

    def m_copies(r):
        cols = pl.ds(column(r), cw)
        return (
            pltpu.make_async_copy(m1_hbm.at[0, :, cols], m1.at[r], m_sem.at[0, r]),
            pltpu.make_async_copy(m2_hbm.at[0, :, cols], m2.at[r], m_sem.at[1, r]),
            pltpu.make_async_copy(
                w_hbm.at[pl.ds(pl.multiple_of(dp * rows, rows), rows), cols], master.at[r], m_sem.at[2, r]
            ),
        )

    def remote(src, dst, send_sem, recv_sem, device):
        return pltpu.make_async_remote_copy(
            src_ref=src, dst_ref=dst, send_sem=send_sem, recv_sem=recv_sem,
            device_id=device, device_id_type=MESH,
        )

    def partial_send(c):
        return remote(psend.at[c], precv.at[c], ps_s.at[c], ps_r.at[c], peer_id())

    def stat_send():
        return remote(stat_s, stat_r, st_s, st_r, peer_id())

    def ctx_send():
        return remote(ctx.at[pl.ds(0, tok)], ctx.at[pl.ds(tok, tok)], cx_s, cx_r, bit_id(0))

    def grad_peer(c):
        return remote(
            g.at[c, pl.ds(0, tok)], g.at[half + c, pl.ds(0, tok)], gy_s.at[c], gy_r.at[c], peer_id()
        )

    def grad_mate(r):
        return remote(
            g.at[r, pl.ds(0, tok)], g.at[r, pl.ds(tok, tok)], gm_s.at[r], gm_r.at[r], bit_id(0)
        )

    def shard_send(k, c):
        return remote(
            sends[k - 1].at[c], recvs[k - 1].at[c], rs_s.at[k - 1, c], rs_r.at[k - 1, c], bit_id(k)
        )

    def gain_send(b):
        device = bit_id(b) if b < bits else peer_id()
        return remote(gp.at[b], gpr.at[b], gg_s.at[b], gg_r.at[b], device)

    ctx_copy().start()

    @pl.loop(0, half)
    def _(c):
        w_copy(half + c).start()

    barrier = pltpu.get_barrier_semaphore()
    pl.semaphore_signal(barrier, inc=1, device_id=peer_id(), device_id_type=MESH)
    for bit in range(bits):
        pl.semaphore_signal(barrier, inc=1, device_id=bit_id(bit), device_id_type=MESH)
    pl.semaphore_wait(barrier, bits + 1)

    ctx_copy().wait()
    ctx_send().start()

    @pl.loop(0, half)
    def _(c):
        w_copy(c).start()
        cot_copy(c).start()

    gain_copy().start()

    @pl.loop(0, half)
    def _(c):
        w_copy(half + c).wait()
        psend[c] = jnp.dot(
            ctx[0:tok], wv[half + c], preferred_element_type=F32
        ).astype(BF16)
        partial_send(c).start()

    @pl.loop(0, half)
    def _(c):
        w_copy(c).wait()
        own[c] = jnp.dot(ctx[0:tok], wv[c], preferred_element_type=F32)
        cot_copy(c).wait()

    @pl.loop(0, chunks)
    def _(r):
        for copy in m_copies(r):
            copy.start()

    gain_copy().wait()
    for r in range(chunks):
        gain[r] = gain_flat[r * cw:(r + 1) * cw].reshape(1, cw)

    ctx_send().wait_recv()
    ctxt_all[...] = jnp.transpose(ctx[...].astype(F32)).reshape(n, rows, 2 * tok)
    blocks = []
    for place in range(n // 2):
        shard = dp
        for k in range(1, bits):
            if not (place >> (bits - 1 - k)) & 1:
                shard = flip(shard, k)
        blocks.append(ctxt_all[shard])
    ctxt[...] = jnp.concatenate(blocks, axis=0).astype(BF16)

    def fold(value):
        total = value[:, 0:128]
        for lane in range(128, cw, 128):
            total = total + value[:, lane:lane + 128]
        return total

    def gather_stats(c, carry):
        square, cross = carry
        partial_send(c).wait_recv()
        attn = own[c] + precv[c].astype(F32)
        own[c] = attn
        scaled = cot[c].astype(F32) * gain[mp * half + c]
        return square + fold(attn * attn), cross + fold(scaled * attn)

    zero = jnp.zeros((tok, 128), F32)
    square, cross = lax.fori_loop(0, half, gather_stats, (zero, zero))
    square = jnp.sum(square, axis=1, keepdims=True)
    cross = jnp.sum(cross, axis=1, keepdims=True)
    even = lax.broadcasted_iota(jnp.int32, (tok, 128), 1) % 2 == 0
    stat_s[...] = jnp.transpose(jnp.where(even, square, cross))[0:8]
    stat_send().start()
    stat_send().wait_recv()
    totals = jnp.transpose(jnp.concatenate([stat_s[...] + stat_r[...]] * 16, axis=0))
    inverse = lax.rsqrt(totals[:, 0:1] / width + norm_floor)
    shift = inverse * totals[:, 1:2] / width

    @pl.loop(0, half)
    def _(c):
        upstream = cot[c].astype(F32)
        normed = own[c] * inverse
        g[c, 0:tok] = (inverse * (upstream * gain[mp * half + c] - normed * shift)).astype(BF16)
        grad_peer(c).start()
        grad_mate(c).start()
        gp[0, c] = jnp.sum(upstream * normed, axis=0, keepdims=True)

    gc_acc[...] = jnp.zeros_like(gc_acc)
    gain_send(0).start()

    n_final = chunks + LAG * (bits - 1)

    @pl.loop(0, max(n_final, bits + 3))
    def _(t):
        ahead = t + AHEAD

        @pl.when((ahead >= half) & (ahead < chunks))
        def _():
            grad_peer(ahead - half).wait_recv()
            grad_mate(ahead).start()

        @pl.when(t < chunks)
        def _():
            grad_mate(t).wait_recv()
            product = jnp.dot(ctxt[...], g[t], preferred_element_type=F32)
            cut = product.shape[0] // 2
            sends[0][t] = product[:cut].astype(BF16)
            shard_send(1, t).start()
            keeps[0][t] = product[cut:]
            gc_acc[...] += lax.dot_general(
                g[t, 0:tok], wv[t], (((1,), (1,)), ((), ())), preferred_element_type=F32
            )

        @pl.when(t == chunks)
        def _():
            gc_out[...] = gc_acc[...].astype(BF16)

        for b in range(bits + 1):
            @pl.when(t == b + 1)
            def _():
                gain_send(b).wait_recv()
                if b < bits:
                    gp[b + 1] = gp[b] + gpr[b]
                    gain_send(b + 1).start()
                else:
                    gfin[pl.ds(mp * half, half)] = gp[bits]
                    gfin[pl.ds(peer * half, half)] = gpr[bits]

        for k in range(bits - 1, 0, -1):
            c = t - LAG * k

            @pl.when((c >= 0) & (c < chunks))
            def _():
                shard_send(k, c).wait_recv()
                total = keeps[k - 1][c] + recvs[k - 1][c].astype(F32)
                if k < bits - 1:
                    cut = total.shape[0] // 2
                    sends[k][c] = total[:cut].astype(BF16)
                    shard_send(k + 1, c).start()
                    keeps[k][c] = total[cut:]
                else:
                    for copy in m_copies(c):
                        copy.wait()
                    first = beta_one * m1[c] + (1.0 - beta_one) * total
                    second = beta_two * m2[c] + (1.0 - beta_two) * total * total
                    cols = pl.ds(column(c), cw)
                    nw[0, :, cols] = (
                        master[c].astype(F32) - learn_rate * first / (jnp.sqrt(second) + adam_floor)
                    ).astype(BF16)
                    n1[0, :, cols] = first
                    n2[0, :, cols] = second

    ctx_send().wait_send()
    stat_send().wait_send()

    @pl.loop(0, half)
    def _(c):
        partial_send(c).wait_send()
        grad_peer(c).wait_send()

    for b in range(bits + 1):
        gain_send(b).wait_send()

    @pl.loop(0, chunks)
    def _(r):
        grad_mate(r).wait_send()
        for k in range(1, bits):
            shard_send(k, r).wait_send()


def settle(nw, n1, n2, gg, gc, nw_out, n1_out, n2_out, gg_out, gc_out, flat, sem):
    pairs = ((nw, nw_out), (n1, n1_out), (n2, n2_out), (gc, gc_out))
    copies = [pltpu.make_async_copy(a, b, sem.at[i]) for i, (a, b) in enumerate(pairs)]
    for copy in copies:
        copy.start()
    chunks, _, cw = gg.shape
    for r in range(chunks):
        flat[r * cw:(r + 1) * cw] = gg[r].reshape(cw)
    copies.append(pltpu.make_async_copy(flat, gg_out, sem.at[4]))
    copies[-1].start()
    for copy in copies:
        copy.wait()


def per_device(n, context, out_weight, cotangent, norm_gain, first_moment, second_moment):
    tok, heads = context.shape
    width = out_weight.shape[1]
    rows = first_moment.shape[1]
    bits = n.bit_length() - 1
    cw = 256
    half = width // (2 * cw)
    chunks = 2 * half
    cfg = (n, bits, half, chunks, cw, rows, tok, heads, width)
    sizes = [(n >> (k + 1)) * rows for k in range(1, bits)]
    dma = pltpu.SemaphoreType.DMA
    vmem = pltpu.VMEM
    scratch = [
        vmem((chunks, heads, cw), BF16),
        vmem((2 * tok, heads), BF16),
        vmem((n, rows, 2 * tok), F32),
        vmem((heads // 2, 2 * tok), BF16),
        vmem((half, tok, cw), BF16),
        vmem((width,), F32),
        vmem((chunks, 1, cw), F32),
        vmem((half, tok, cw), BF16),
        vmem((half, tok, cw), BF16),
        vmem((half, tok, cw), F32),
        vmem((8, tok), F32),
        vmem((8, tok), F32),
        vmem((chunks, 2 * tok, cw), BF16),
        tuple(vmem((chunks, size, cw), BF16) for size in sizes),
        tuple(vmem((chunks, size, cw), BF16) for size in sizes),
        tuple(vmem((chunks, size, cw), F32) for size in sizes),
        vmem((chunks, rows, cw), F32),
        vmem((chunks, rows, cw), F32),
        vmem((chunks, rows, cw), BF16),
        vmem((tok, heads), F32),
        vmem((bits + 1, half, 1, cw), F32),
        vmem((bits + 1, half, 1, cw), F32),
        dma((2,)), dma((chunks,)), dma((half,)), dma((3, chunks)),
        dma((half,)), dma((half,)), dma, dma, dma, dma,
        dma((half,)), dma((half,)), dma((chunks,)), dma((chunks,)),
        dma((bits - 1, chunks)), dma((bits - 1, chunks)), dma((bits + 1,)), dma((bits + 1,)),
    ]
    anywhere = pl.BlockSpec(memory_space=pltpu.HBM)
    new_weight, new_first, new_second, grad_gain, grad_context = pl.pallas_call(
        functools.partial(kernel, cfg),
        out_shape=(
            jax.ShapeDtypeStruct(first_moment.shape, BF16),
            jax.ShapeDtypeStruct(first_moment.shape, F32),
            jax.ShapeDtypeStruct(first_moment.shape, F32),
            jax.ShapeDtypeStruct((chunks, 1, cw), F32),
            jax.ShapeDtypeStruct((tok, heads), BF16),
        ),
        in_specs=[anywhere] * 6,
        out_specs=(pl.BlockSpec(memory_space=pltpu.VMEM),) * 5,
        scratch_shapes=scratch,
        compiler_params=pltpu.CompilerParams(
            collective_id=0, has_side_effects=True, vmem_limit_bytes=50 * 1024 * 1024
        ),
    )(context, out_weight, cotangent, norm_gain, first_moment, second_moment)
    return pl.pallas_call(
        settle,
        out_shape=(
            jax.ShapeDtypeStruct(first_moment.shape, BF16),
            jax.ShapeDtypeStruct(first_moment.shape, F32),
            jax.ShapeDtypeStruct(first_moment.shape, F32),
            jax.ShapeDtypeStruct((width,), F32),
            jax.ShapeDtypeStruct((tok, heads), BF16),
        ),
        in_specs=[pl.BlockSpec(memory_space=pltpu.VMEM)] * 5,
        out_specs=(anywhere,) * 5,
        scratch_shapes=[vmem((width,), F32), dma((5,))],
        compiler_params=pltpu.CompilerParams(vmem_limit_bytes=8 * 1024 * 1024),
    )(new_weight, new_first, new_second, grad_gain, grad_context)


def solution(mesh):
    return jax.shard_map(
        functools.partial(per_device, mesh.shape["dp"]),
        mesh=mesh,
        in_specs=(
            P("dp", "mp"),
            P("mp", None),
            P("dp", None),
            P(),
            P("mp", "dp", None),
            P("mp", "dp", None),
        ),
        out_specs=(
            P("mp", "dp", None),
            P("mp", "dp", None),
            P("mp", "dp", None),
            P(),
            P("dp", "mp"),
        ),
        check_vma=False,
    )
```
